512 devices in a mesh: shot: 8 (over z), mp: 64 (over x, y, core).
Axes of the slice: x: 4, y: 8, z: 8, core: 2. Of those that a mesh axis runs over, the one named last changes fastest.
Arguments:
- gradient_parts: float32 [32, 4096, 1024], P('shot', 'mp')
- history_s: bfloat16 [10, 4096, 1024], P(None, 'mp'), may hold values from -6 to 6
- history_y: bfloat16 [10, 4096, 1024], P(None, 'mp'), as said below
Outputs:
- direction: float32 [4096, 1024], P('mp', 'shot')
The draws below stay inside these ranges and needn't reach their ends.
Inputs may be any that keep to these rules, and one draw needn't show every extreme that they name: In every cell, history_y[i] equals history_s[i] times a factor between 0.5 and 4.
All inputs are finite; a program needn't handle non-finite values.
Results may differ from the reference program's by a relative error of at most 0.0003.
Values sent between devices are 32-bit elements; how exact they have to be, the bound alone decides.
A program may use at most 64 MiB of HBM per device.

```python
import jax
import jax.numpy as jnp
from jax import lax

M = 10
SHOT_DEV = 4
WIDTH = 1024
ROWS = 4096
N_SHOT = 8


def basis(key):
    keys = jax.random.split(jax.random.fold_in(key, 11), 2)
    ramp = jnp.exp(jnp.log(3.0) * jnp.arange(ROWS, dtype=jnp.float32) / (ROWS - 1))[None, :, None]
    steps = jnp.clip(jax.random.normal(keys[0], (M, ROWS, WIDTH), jnp.float32), -2.0, 2.0)
    steps = steps * ramp
    factor = jnp.exp(jax.random.uniform(keys[1], (M, ROWS, WIDTH), jnp.float32, -0.69, 1.38))
    return (steps, factor * steps)


def draw_history_s(key, part):
    return basis(key)[0].astype(jnp.bfloat16)


def draw_history_y(key, part):
    return basis(key)[1].astype(jnp.bfloat16)


def draw_gradient_parts(key, part):
    steps, changes = basis(key)
    keys = jax.random.split(jax.random.fold_in(key, 23), 3)
    mix_s = jax.random.normal(keys[0], (M,), jnp.float32) / (2.0 * M) ** 0.5
    mix_y = jax.random.normal(keys[1], (M,), jnp.float32) / (2.0 * M) ** 0.5
    common = jnp.einsum('m,mrc->rc', mix_s, steps, precision=lax.Precision.HIGHEST)
    common = common + jnp.einsum('m,mrc->rc', mix_y, changes, precision=lax.Precision.HIGHEST)
    total = SHOT_DEV * N_SHOT
    ramp = 1.0 + 2.0 * jnp.arange(total, dtype=jnp.float32) / (total - 1)
    noise = jax.random.normal(keys[2], (total, ROWS, WIDTH), jnp.float32)
    return ramp[:, None, None] * (common[None] / total + 0.5 / total ** 0.5 * noise)


def setup_inputs(seed: int = 0) -> dict:
    splits = jax.random.split(jax.random.key(seed), 4)
    return {
        "gradient_parts": draw_gradient_parts(jax.random.fold_in(splits[3], 71), 0),
        "history_s": draw_history_s(jax.random.fold_in(splits[3], 71), 0),
        "history_y": draw_history_y(jax.random.fold_in(splits[3], 71), 0),
    }


def inner(left, right):
    return jnp.sum(left.astype(jnp.float32) * right.astype(jnp.float32))


def reference(gradient_parts, history_s, history_y):
    gradient = jnp.sum(gradient_parts, axis=0)
    rho = [1.0 / inner(history_s[i], history_y[i]) for i in range(M)]
    gamma = inner(history_s[M - 1], history_y[M - 1]) / inner(history_y[M - 1], history_y[M - 1])
    q_vec = gradient
    alphas = [None] * M
    for i in reversed(range(M)):
        alphas[i] = rho[i] * inner(history_s[i], q_vec)
        q_vec = q_vec - alphas[i] * history_y[i].astype(jnp.float32)
    r_vec = gamma * q_vec
    for i in range(M):
        beta = rho[i] * inner(history_y[i], r_vec)
        r_vec = r_vec + (alphas[i] - beta) * history_s[i].astype(jnp.float32)
    return -r_vec
```

```python
import functools

import jax
import jax.numpy as jnp
from jax import lax
from jax.experimental import pallas as pl
from jax.experimental.pallas import tpu as pltpu
from jax.sharding import Mesh
from jax.sharding import PartitionSpec as P

M = 10
MP = ("mp_0", "mp_1", "mp_2")
MESH = pl.DeviceIdType.MESH
CHUNK = 16
GROUP = 72
PAIRS = [(i, j) for i in range(M) for j in range(i, M)]
ROW = {pair: k for k, pair in enumerate(PAIRS)}
CROSS = len(PAIRS)


def folded(x):
    rows = x.shape[0]
    parts = [x[8 * t : 8 * t + 8] for t in range(rows // 8)]
    while len(parts) > 1:
        parts = [a + b for a, b in zip(parts[::2], parts[1::2])]
    return parts[0]


def kernel(
    sizes,
    parts_hbm,
    s_hbm,
    y_hbm,
    out_ref,
    parts_v,
    s_v,
    y_v,
    part_v,
    got_v,
    mine_v,
    acc_v,
    wide_v,
    msg_v,
    in_v,
    load_sem,
    g_send,
    g_recv,
    m_send,
    m_recv,
):
    nz, nx, ny, nc = sizes
    z, x, y, c = (lax.axis_index(name) for name in ("shot", *MP))
    rows = s_v.shape[1]
    width = s_v.shape[2]
    cols = width // nz
    chunks = rows // CHUNK

    def load(k, src, dst, which):
        span = pl.ds(k * CHUNK, CHUNK)
        return pltpu.make_async_copy(
            src.at[:, span, :], dst.at[:, span, :], load_sem.at[which, k]
        )

    for k in range(chunks):
        load(k, parts_hbm, parts_v, 0).start()
    for k in range(chunks):
        load(k, s_hbm, s_v, 1).start()
        load(k, y_hbm, y_v, 2).start()

    stages = (
        [
            {"mp_0": lax.rem(x + dx, nx), "mp_2": lax.rem(c + dc, nc)}
            for dx in range(nx)
            for dc in range(nc)
            if dx + dc
        ],
        [{"mp_1": lax.rem(y + d, ny)} for d in range(1, ny)],
        [{"shot": lax.rem(z + d, nz)} for d in range(1, nz)],
    )

    def device(where):
        here = {"shot": z, "mp_0": x, "mp_1": y, "mp_2": c}
        here.update(where)
        return (here["shot"], here["mp_0"], here["mp_1"], here["mp_2"])

    barrier = pltpu.get_barrier_semaphore()
    for stage in stages:
        for where in stage:
            pl.semaphore_signal(
                barrier, inc=1, device_id=device(where), device_id_type=MESH
            )

    for k in range(chunks):
        load(k, parts_hbm, parts_v, 0).wait()
        span = pl.ds(k * CHUNK, CHUNK)
        total = parts_v[0, span, :]
        for shot in range(1, parts_v.shape[0]):
            total = total + parts_v[shot, span, :]
        for block in range(nz):
            part_v[block, span, :] = total[:, block * cols : (block + 1) * cols]

    def cross(k, sums):
        load(k, s_hbm, s_v, 1).wait()
        load(k, y_hbm, y_v, 2).wait()
        span = pl.ds(pl.multiple_of(k * CHUNK, CHUNK), CHUNK)
        grads = [part_v[block, span, :] for block in range(nz)]
        new = []
        for n, acc in enumerate(sums):
            vec = s_v if n < M else y_v
            values = vec[n % M, span, :].astype(jnp.float32)
            prods = [
                values[:, block * cols : (block + 1) * cols] * grads[block]
                for block in range(nz)
            ]
            while len(prods) > 1:
                prods = [a + b for a, b in zip(prods[::2], prods[1::2])]
            new.append(acc + folded(prods[0]))
        return tuple(new)

    zero = jnp.zeros((8, cols), jnp.float32)
    sums = lax.fori_loop(0, chunks, cross, (zero,) * (2 * M))
    for n in range(2 * M):
        at = (n // M) * GROUP + CROSS + n % M
        acc_v[8 * at : 8 * at + 8, :] = sums[n]
    for group in range(2):
        for at in range(group * GROUP + CROSS + M, (group + 1) * GROUP):
            acc_v[8 * at : 8 * at + 8, :] = zero

    own = pl.ds(pl.multiple_of(z * cols, cols), cols)
    for n in range(M):
        mine_v[n] = s_v[n, :, own].astype(jnp.float32)
        mine_v[M + n] = y_v[n, :, own].astype(jnp.float32)
    for (i, j), at in ROW.items():
        right = mine_v[M + j]
        acc_v[8 * at : 8 * at + 8, :] = folded(mine_v[i] * right)
        at = at + GROUP
        acc_v[8 * at : 8 * at + 8, :] = folded(mine_v[M + i] * right)

    slabs = [acc_v[pl.ds(r, 2 * GROUP, stride=8), :] for r in range(8)]
    while len(slabs) > 1:
        slabs = [a + b for a, b in zip(slabs[::2], slabs[1::2])]
    lanes = jnp.sum(slabs[0], axis=1, keepdims=True)
    eye = lax.broadcasted_iota(jnp.int32, (GROUP, cols), 0) == lax.broadcasted_iota(
        jnp.int32, (GROUP, cols), 1
    )
    for group in range(2):
        column = lanes[group * GROUP : (group + 1) * GROUP]
        line = jnp.where(eye, jnp.broadcast_to(column, (GROUP, cols)), 0.0)
        msg_v[0, group : group + 1, :] = jnp.sum(line, axis=0, keepdims=True)

    pl.semaphore_wait(barrier, sum(len(stage) for stage in stages))

    def share(n, d):
        return pltpu.make_async_remote_copy(
            src_ref=msg_v.at[n],
            dst_ref=in_v.at[n, d],
            send_sem=m_send.at[n, d],
            recv_sem=m_recv.at[n, d],
            device_id=device(stages[n][d]),
            device_id_type=MESH,
        )

    def give(d):
        return pltpu.make_async_remote_copy(
            src_ref=part_v.at[lax.rem(z + d + 1, nz)],
            dst_ref=got_v.at[d],
            send_sem=g_send.at[d],
            recv_sem=g_recv.at[d],
            device_id=device(stages[2][d]),
            device_id_type=MESH,
        )

    for d in range(len(stages[0])):
        share(0, d).start()
    for d in range(nz - 1):
        give(d).start()

    for n in range(3):
        count = len(stages[n])
        if n == 2:
            grad = part_v[z]
            for d in range(nz - 1):
                give(d).wait_recv()
                grad = grad + got_v[d]
        total = msg_v[n]
        for d in range(count):
            share(n, d).wait_recv()
            total = total + in_v[n, d]
        if n < 2:
            msg_v[n + 1] = total
            for d in range(len(stages[n + 1])):
                share(n + 1, d).start()

    for group in range(2):
        line = jnp.broadcast_to(total[group : group + 1], (GROUP, cols))
        column = jnp.sum(jnp.where(eye, line, 0.0), axis=1, keepdims=True)
        wide_v[group * GROUP : (group + 1) * GROUP, :] = jnp.broadcast_to(
            column, (GROUP, cols)
        )

    def splat(at):
        return jnp.broadcast_to(wide_v[at : at + 1, :], (8, cols))

    sy = {pair: splat(at) for pair, at in ROW.items()}
    yy = {pair: splat(GROUP + at) for pair, at in ROW.items()}
    sg = [splat(CROSS + i) for i in range(M)]
    yg = [splat(GROUP + CROSS + i) for i in range(M)]
    rho = [1.0 / sy[i, i] for i in range(M)]
    gamma = sy[M - 1, M - 1] / yy[M - 1, M - 1]
    alpha = [None] * M
    for i in reversed(range(M)):
        alpha[i] = rho[i] * sg[i]
        for j in range(i):
            sg[j] = sg[j] - alpha[i] * sy[j, i]
        for j in range(M):
            yg[j] = yg[j] - alpha[i] * yy[min(i, j), max(i, j)]
    yg = [gamma * v for v in yg]
    delta = [None] * M
    for i in range(M):
        delta[i] = alpha[i] - rho[i] * yg[i]
        for j in range(i + 1, M):
            yg[j] = yg[j] + delta[i] * sy[i, j]
    shape = (rows // 8, 8, cols)
    back = grad.reshape(shape)
    for i in range(M):
        back = back - alpha[i][None] * mine_v[M + i].reshape(shape)
    back = gamma[None] * back
    for i in range(M):
        back = back + delta[i][None] * mine_v[i].reshape(shape)
    out_ref[...] = -back.reshape(rows, cols)

    for n in range(3):
        for d in range(len(stages[n])):
            share(n, d).wait_send()
    for d in range(nz - 1):
        give(d).wait_send()


def solution(mesh):
    nz, ny, nc = mesh.shape["shot"], 8, 2
    nx = mesh.shape["mp"] // (ny * nc)
    torus = Mesh(mesh.devices.reshape(nz, nx, ny, nc), ("shot", *MP))

    def shards(gradient_parts, history_s, history_y):
        shots, rows, width = gradient_parts.shape
        cols = width // nz
        f32, bf16 = jnp.float32, jnp.bfloat16
        most = max(nx * nc, ny, nz) - 1
        return pl.pallas_call(
            functools.partial(kernel, (nz, nx, ny, nc)),
            out_shape=jax.ShapeDtypeStruct((rows, cols), f32),
            in_specs=[pl.BlockSpec(memory_space=pl.ANY)] * 3,
            out_specs=pl.BlockSpec(memory_space=pltpu.VMEM),
            scratch_shapes=[
                pltpu.VMEM((shots, rows, width), f32),
                pltpu.VMEM((M, rows, width), bf16),
                pltpu.VMEM((M, rows, width), bf16),
                pltpu.VMEM((nz, rows, cols), f32),
                pltpu.VMEM((nz - 1, rows, cols), f32),
                pltpu.VMEM((2 * M, rows, cols), f32),
                pltpu.VMEM((2 * GROUP * 8, cols), f32),
                pltpu.VMEM((2 * GROUP, cols), f32),
                pltpu.VMEM((3, 2, cols), f32),
                pltpu.VMEM((3, most, 2, cols), f32),
                pltpu.SemaphoreType.DMA((3, rows // CHUNK)),
                pltpu.SemaphoreType.DMA((nz - 1,)),
                pltpu.SemaphoreType.DMA((nz - 1,)),
                pltpu.SemaphoreType.DMA((3, most)),
                pltpu.SemaphoreType.DMA((3, most)),
            ],
            compiler_params=pltpu.CompilerParams(collective_id=0, has_side_effects=True),
        )(gradient_parts, history_s, history_y)

    return jax.shard_map(
        shards,
        mesh=torus,
        in_specs=(P("shot", MP, None), P(None, MP, None), P(None, MP, None)),
        out_specs=P(MP, "shot"),
        check_vma=False,
    )
```
